32 devices in a mesh: row: 16 (over z, y, core), col: 2 (over x).
Axes of the slice: x: 2, y: 2, z: 4, core: 2. Of those that a mesh axis runs over, the one named last changes fastest.
Arguments:
- features: bfloat16 [256, 128, 384], P('row', 'col'), may hold values from -30 to 30
- inner_weights: bfloat16 [4, 3, 3, 384, 384], replicated, may hold values from -0.109375 to 0.109375
- far_weights: bfloat16 [3, 3, 384, 384], replicated, may hold values from -0.109375 to 0.109375
- gains: float32 [5, 384], replicated, may hold values from 0.1 to 1.9
Outputs:
- result: float32 [256, 128, 384], P('row', 'col')
The draws below stay inside these ranges and needn't reach their ends.
All inputs are finite; a program needn't handle non-finite values.
Results may differ from the reference program's by a relative error of at most 0.0024.
Values may be sent and summed in bfloat16 or wider, within the bound.
No kernel may reach another device: no remote copies, remote signals or barrier semaphores. Data moves between devices by JAX's collectives and lax.ppermute only.
A program may use at most 192 MiB of HBM per device.

```python
import math
import jax
import jax.numpy as jnp
from jax import lax

CH = 384
LAYERS = 4
FAR = 64
HEIGHT = 256
WIDTH = 128


def draw_features(key, part):
    key_base, key_chan, key_cell = jax.random.split(key, 3)
    channel_scale = jnp.exp(jax.random.uniform(key_chan, (CH,), jnp.float32, math.log(0.3), math.log(3.0)))
    cell_scale = jnp.exp(jax.random.uniform(key_cell, (HEIGHT, WIDTH, 1), jnp.float32, math.log(0.5), math.log(2.0)))
    base_values = jnp.clip(jax.random.normal(key_base, (HEIGHT, WIDTH, CH), jnp.float32), -5.0, 5.0)
    return (base_values * channel_scale * cell_scale).astype(jnp.bfloat16)


def normal_values(stream_key, shape, deviation, most, kind=jnp.bfloat16):
    result = deviation * jax.random.normal(stream_key, shape, jnp.float32)
    return jnp.clip(result, min=-most, max=most).astype(kind)


def setup_inputs(seed: int = 0) -> dict:
    splits = jax.random.split(jax.random.key(seed), 5)
    return {
        "features": draw_features(jax.random.fold_in(splits[4], 71), 0),
        "inner_weights": normal_values(splits[1], (LAYERS, 3, 3, CH, CH), (9 * CH) ** -0.5, 0.109375),
        "far_weights": normal_values(splits[2], (3, 3, CH, CH), (9 * CH) ** -0.5, 0.109375),
        "gains": jnp.clip(1.0 + 0.18 * jax.random.normal(splits[3], (LAYERS + 1, CH), jnp.float32), 0.1, 1.9),
    }


dilation_steps = (1, 2, 4, 8)

def norm_act(stream, scale_gain):
    centre = lax.optimization_barrier(jnp.mean(stream, axis=-1, keepdims=True))
    spread = lax.optimization_barrier(jnp.mean((stream - centre) * (stream - centre), axis=-1, keepdims=True))
    normed = (stream - centre) * lax.rsqrt(spread + 1e-05) * scale_gain
    return jax.nn.gelu(normed).astype(jnp.bfloat16)

def dilated(activated, kernel, dilation):
    output = lax.conv_general_dilated(activated[None], kernel, (1, 1), ((dilation, dilation), (dilation, dilation)), rhs_dilation=(dilation, dilation), dimension_numbers=('NHWC', 'HWIO', 'NHWC'), preferred_element_type=jnp.float32)
    return output[0].astype(jnp.float32)

def reference(features, inner_weights, far_weights, gains):
    stream = features.astype(jnp.float32)
    for layer in range(LAYERS):
        dilation = dilation_steps[layer]
        stream = stream + dilated(norm_act(stream, gains[layer]), inner_weights[layer], dilation)
    stream = stream + dilated(norm_act(stream, gains[LAYERS]), far_weights, FAR)
    return stream
```

```python
import functools

import jax
import jax.numpy as jnp
from jax import lax
from jax.experimental import pallas as pl
from jax.experimental.pallas import tpu as pltpu
from jax.sharding import PartitionSpec as P

FAR = 64
DILATIONS = (1, 2, 4, 8)
PAD = 8
VMEM_LIMIT = 40 * 1024 * 1024


def normed(stream, gain):
    centre = jnp.mean(stream, axis=-1, keepdims=True)
    moved = stream - centre
    spread = jnp.mean(moved * moved, axis=-1, keepdims=True)
    return jax.nn.gelu(moved * lax.rsqrt(spread + 1e-05) * gain)


def spread_taps(line_ref, taps_ref, row, dilation, start, cols):
    ch = line_ref.shape[-1]
    for tap in range(3):
        shift = (tap - 1) * dilation
        taps_ref[row, :, tap * ch : (tap + 1) * ch] = line_ref[row, pl.ds(start + shift, cols), :].astype(
            taps_ref.dtype
        )


def clear_edges(line_ref):
    rows, width, ch = line_ref.shape
    line_ref[:, 0:PAD, :] = jnp.zeros((rows, PAD, ch), line_ref.dtype)
    line_ref[:, width - PAD : width, :] = jnp.zeros((rows, PAD, ch), line_ref.dtype)


def conv_part(taps_ref, weight_ref, first, rows, dilation, taps=(0, 1, 2)):
    cols, depth = taps_ref.shape[1:]
    lhs = [taps_ref[first + tap * dilation : first + tap * dilation + rows].reshape(rows * cols, depth) for tap in taps]
    lhs = lhs[0] if len(lhs) == 1 else jnp.concatenate(lhs, axis=1)
    weight = weight_ref[taps[0] * depth : (taps[-1] + 1) * depth, :]
    out = jnp.dot(lhs, weight, preferred_element_type=jnp.float32)
    return out.reshape(rows, cols, out.shape[-1])


def in_grid(col_lo, col_hi, value):
    cols = lax.broadcasted_iota(jnp.int32, value.shape, 0)
    keep = (cols >= col_lo) & (cols < col_hi)
    return jnp.where(keep, value, 0.0)


class Plan:
    def __init__(self, tile_rows, tile_cols, ch, n_row, n_col):
        self.tile_rows, self.tile_cols, self.ch = tile_rows, tile_cols, ch
        self.n_row, self.n_col = n_row, n_col
        self.two = n_col == 2
        self.ext = -(-sum(DILATIONS) // 16) * 16
        self.width = tile_cols + (self.ext if self.two else 2 * self.ext)
        self.last = DILATIONS[-1]
        self.width4 = tile_cols + (self.last if self.two else 2 * self.last)

    def own(self, col):
        return pl.multiple_of(col * self.ext, 8) if self.two else self.ext

    def own4(self, col):
        return pl.multiple_of(col * self.last, 8) if self.two else self.last

    def start4(self, col):
        return pl.multiple_of(col * (self.ext - self.last), 8) if self.two else self.ext - self.last

    def sides(self, col):
        if self.two:
            return (pl.multiple_of((1 - col) * self.tile_cols, 8),)
        return (0, self.ext + self.tile_cols)

    def col_range(self, col):
        if self.two:
            return 0, self.width
        lo = jnp.where(col == 0, self.ext, 0)
        hi = jnp.where(col == self.n_col - 1, self.ext + self.tile_cols, self.width)
        return lo, hi

    def inside(self, col, value):
        if self.two:
            return value
        return in_grid(*self.col_range(col), value)

    def starts(self, row_id, span):
        last = self.tile_rows - span
        one = jnp.where(row_id % 2 == 0, last, 0)
        return one, last - one


def lay(line, taps, row, value, dilation, start, cols):
    width = value.shape[0]
    line[row, PAD : PAD + width, :] = value
    spread_taps(line, taps, row, dilation, start, cols)


def rows_of(count, body, step=4):
    def block(k, _):
        for j in range(step):
            body(k * step + j)
        return 0

    lax.fori_loop(0, count // step, block, 0)
    for row in range(count // step * step, count):
        body(row)


def gather_rows(plan, halo, features, *refs):
    n_side = 1 if plan.two else 2
    sides, outs, (sems,) = refs[:n_side], refs[n_side : n_side + 2], refs[n_side + 2 :]
    row_id, col = lax.axis_index("row"), lax.axis_index("col")
    copies = []
    for out, start in zip(outs, plan.starts(row_id, halo)):
        for part, offset in zip((features,) + sides, (plan.own(col),) + plan.sides(col)):
            copies.append(
                pltpu.make_async_copy(
                    part.at[pl.ds(start, halo)],
                    out.at[:, pl.ds(offset, part.shape[1])],
                    sems.at[len(copies)],
                )
            )
    for copy in copies:
        copy.start()
    for copy in copies:
        copy.wait()


CHUNK = 4


def one_own(plan, halo, *refs):
    n_side = 1 if plan.two else 2
    parts = refs[: 1 + n_side]
    w_hbm, gains, mid, mid_act, edge_act, edge_base, base, line, taps, weight, sem = refs[1 + n_side :]
    col = lax.axis_index("col")
    copy = pltpu.make_async_copy(w_hbm.at[0], weight, sem)
    copy.start()
    rows, width = plan.tile_rows, plan.width
    for part, offset in zip(parts, (plan.own(col),) + plan.sides(col)):
        base[:, pl.ds(offset, part.shape[1]), :] = part[...].astype(jnp.float32)
    clear_edges(line)

    def prepare(row):
        lay(line, taps, row, plan.inside(col, normed(base[row], gains[0:1, :])), DILATIONS[0], PAD, width)

    def follow(row):
        mid_act[row] = plan.inside(col, normed(mid[row], gains[1:2, :])).astype(mid_act.dtype)

    lead = 2 * CHUNK
    rows_of(lead, prepare)
    copy.wait()
    edge = DILATIONS[1]
    count = mid.shape[0] // CHUNK
    for k in range(count):
        at = k * CHUNK
        mid[at : at + CHUNK] = base[edge + at : edge + at + CHUNK] + conv_part(
            taps, weight, edge + at - DILATIONS[0], CHUNK, DILATIONS[0]
        )
        for row in range(lead + at, min(lead + at + CHUNK, rows)):
            prepare(row)
        if k:
            for row in range(at - CHUNK, at):
                follow(row)
    ch = plan.ch
    for k, first in enumerate((0, rows - halo)):
        edge_act[k * halo : (k + 1) * halo] = taps[first : first + halo, :, ch : 2 * ch]
        edge_base[k * halo : (k + 1) * halo] = base[first : first + halo]
    rows_of(CHUNK, lambda row: follow((count - 1) * CHUNK + row))


def one_two(plan, halo, *refs):
    got, refs = refs[:2], refs[2:]
    mid, mid_act, edge_act, edge_base, w_hbm, gains, stream, act, send_one, send_two = refs[:10]
    base, line, taps_one, rim, taps_two, w_one, w_two, sems = refs[10:]
    row_id, col = lax.axis_index("row"), lax.axis_index("col")
    copies = [pltpu.make_async_copy(w_hbm.at[k], w, sems.at[k]) for k, w in enumerate((w_one, w_two))]
    for copy in copies:
        copy.start()
    rows, width, ch = plan.tile_rows, plan.width, plan.ch
    d_one, d_two = DILATIONS[:2]
    clear_edges(line)
    base[halo : 3 * halo] = edge_base[...]
    top = (halo * 3) * (1 - row_id % 2)
    for ref, at in zip(got, (top, 3 * halo - top)):
        base[pl.ds(at, halo)] = ref[...].astype(jnp.float32)
    for row in range(2 * halo):
        lay(line, taps_one, halo + row, edge_act[row].astype(jnp.float32), d_one, PAD, width)
    for row in tuple(range(halo)) + tuple(range(3 * halo, 4 * halo)):
        lay(line, taps_one, row, plan.inside(col, normed(base[row], gains[0:1, :])), d_one, PAD, width)
    n_mid = mid.shape[0]

    def spread_mid(row):
        lay(line, taps_two, 2 * d_two + row, mid_act[row].astype(jnp.float32), d_two, PAD, width)

    copies[0].wait()
    for k in range(2):
        at = 2 * halo * k
        rim[k * CHUNK : (k + 1) * CHUNK] = base[at + 1 : at + 1 + CHUNK] + conv_part(taps_one, w_one, at, CHUNK, d_one)
        for row in range(k * n_mid // 2, (k + 1) * n_mid // 2):
            spread_mid(row)
    copies[1].wait()

    def spread_rim(row):
        value = plan.inside(col, normed(rim[row], gains[1:2, :]))
        if row < d_two:
            value = jnp.where(row_id == 0, 0.0, value)
        if row >= 2 * CHUNK - d_two:
            value = jnp.where(row_id == plan.n_row - 1, 0.0, value)
        lay(line, taps_two, row if row < CHUNK else n_mid + row, value, d_two, PAD, width)

    def finish(row):
        act[row] = plan.inside(col, normed(stream[row], gains[2:3, :])).astype(act.dtype)

    def second(first):
        return conv_part(taps_two, w_two, first, CHUNK, d_two)

    inner = tuple(range(CHUNK, rows - CHUNK, CHUNK))
    per = -(-2 * CHUNK // len(inner))
    for k, first in enumerate(inner):
        stream[first : first + CHUNK] = mid[first - d_two : first - d_two + CHUNK] + second(first)
        for row in range(k * per, min((k + 1) * per, 2 * CHUNK)):
            spread_rim(row)
    out = second(0)
    stream[0:d_two] = rim[d_two : 2 * d_two] + out[:d_two]
    stream[d_two:CHUNK] = mid[0 : CHUNK - d_two] + out[d_two:]
    for first in inner[: len(inner) // 2]:
        for row in range(first, first + CHUNK):
            finish(row)
    last = rows - CHUNK
    out = second(last)
    stream[last : last + d_two] = mid[n_mid - d_two : n_mid] + out[:d_two]
    stream[last + d_two : rows] = rim[CHUNK : CHUNK + d_two] + out[d_two:]
    for first in inner[len(inner) // 2 :]:
        for row in range(first, first + CHUNK):
            finish(row)
    rows_of(CHUNK, finish)
    rows_of(CHUNK, lambda row: finish(last + row))
    for ref, at in zip((send_one, send_two), plan.starts(row_id, DILATIONS[2])):
        ref[...] = act[pl.ds(at, DILATIONS[2])]


def three_own(plan, act, w_hbm, stream, gains, edge, mid, mid_act, line, taps, full, row_act, weight, sem):
    col = lax.axis_index("col")
    copy = pltpu.make_async_copy(w_hbm.at[2], weight, sem)
    copy.start()
    d = DILATIONS[2]
    rows, width = plan.tile_rows, plan.width
    clear_edges(line)
    rows_of(rows, lambda row: lay(line, taps, row, act[row].astype(jnp.float32), d, PAD, width))
    copy.wait()
    for first in range(d, rows - d, CHUNK):
        full[first - d : first - d + CHUNK] = stream[first : first + CHUNK] + conv_part(taps, weight, first - d, CHUNK, d)

    def finish(row):
        emit(plan, col, full, row_act, row, gains[3:4, :], mid, mid_act, row)

    count = rows - 2 * d
    edge[0:d] = stream[0:d] + conv_part(taps, weight, -d, d, d, (1, 2))
    for row in range(count // 2):
        finish(row)
    edge[d : 2 * d] = stream[rows - d : rows] + conv_part(taps, weight, rows - 2 * d, d, d, (0, 1))
    for row in range(count // 2, count):
        finish(row)


def emit(plan, col, full, row_act, row, gain, stream, act, at):
    row_act[row] = plan.inside(col, normed(full[row], gain))
    act[at] = row_act[row, pl.ds(plan.start4(col), plan.width4), :].astype(act.dtype)
    stream[at] = full[row, pl.ds(plan.own(col), plan.tile_cols), :]


def partner_weights(plan, row_id, w_hbm, layer, weight, sems):
    depth = weight.shape[1]
    one = jnp.where(row_id % 2 == 0, 2 * depth, 0)
    return [
        pltpu.make_async_copy(
            w_hbm.at[layer, pl.ds(pl.multiple_of(at, 16), depth)], weight.at[k], sems.at[k]
        )
        for k, at in enumerate((one, 2 * depth - one))
    ]


def three_rim(plan, got_one, got_two, edge, mid, mid_act, w_hbm, gains, stream, act, send_one, send_two, *scratch):
    line, taps, weight, full, row_act, sems = scratch
    row_id, col = lax.axis_index("row"), lax.axis_index("col")
    copies = partner_weights(plan, row_id, w_hbm, 2, weight, sems)
    for copy in copies:
        copy.start()
    d = DILATIONS[2]
    rows, width = plan.tile_rows, plan.width
    clear_edges(line)
    for k, ref in enumerate((got_one, got_two)):
        for row in range(d):
            lay(line, taps, k * d + row, ref[row].astype(jnp.float32), d, PAD, width)
    stream[d : rows - d] = mid[...]
    act[d : rows - d] = mid_act[...]
    at_one, at_two = plan.starts(row_id, d)
    half = jnp.where(row_id % 2 == 0, d, 0)
    for k, (place, at) in enumerate(((half, at_one), (d - half, at_two))):
        copies[k].wait()
        full[k * d : (k + 1) * d] = edge[pl.ds(place, d)] + conv_part(taps, weight.at[k], k * d, d, d, (0,))
    for k, at in enumerate((at_one, at_two)):
        for row in range(d):
            emit(plan, col, full, row_act, k * d + row, gains[3:4, :], stream, act, at + row)
    for ref, at in zip((send_one, send_two), plan.starts(row_id, DILATIONS[3])):
        ref[...] = act[pl.ds(at, DILATIONS[3])]


def four_own(plan, act, w_hbm, stream, out, line, taps, weight, sem):
    col = lax.axis_index("col")
    copy = pltpu.make_async_copy(w_hbm.at[3], weight, sem)
    copy.start()
    d = DILATIONS[3]
    rows, cols = plan.tile_rows, plan.tile_cols
    start = PAD + plan.own4(col)
    clear_edges(line)
    rows_of(rows, lambda row: lay(line, taps, row, act[row].astype(jnp.float32), d, start, cols))
    copy.wait()
    for first in range(0, rows, CHUNK):
        used = tuple(t for t in range(3) if 0 <= first + (t - 1) * d < rows)
        out[first : first + CHUNK] = stream[first : first + CHUNK] + conv_part(taps, weight, first - d, CHUNK, d, used)


def four_rim(plan, got_one, got_two, acc, w_hbm, gains, stream, act_a, act_b, line, taps, weight, sems):
    row_id, col = lax.axis_index("row"), lax.axis_index("col")
    copies = partner_weights(plan, row_id, w_hbm, 3, weight, sems)
    for copy in copies:
        copy.start()
    d = DILATIONS[3]
    rows, cols = plan.tile_rows, plan.tile_cols
    start = PAD + plan.own4(col)
    clear_edges(line)
    for k, ref in enumerate((got_one, got_two)):
        rows_of(d, lambda row, k=k, ref=ref: lay(line, taps, k * d + row, ref[row].astype(jnp.float32), d, start, cols))
    if rows > 2 * d:
        stream[d : rows - d] = acc[d : rows - d]
    pending = []
    for k, at in enumerate(plan.starts(row_id, d)):
        copies[k].wait()
        for step in range(0, d, CHUNK):
            stream[pl.ds(at + step, CHUNK)] = acc[pl.ds(at + step, CHUNK)] + conv_part(
                taps, weight.at[k], k * d + step, CHUNK, d, (0,)
            )
    half = rows // 2
    for k, act in enumerate((act_a, act_b)):

        def finish(row, act=act, k=k):
            act[row] = normed(stream[k * half + row], gains[4:5, :]).astype(act.dtype)

        rows_of(half, finish)


def times(a, w):
    rows, cols, ch = a.shape
    return jnp.dot(a.reshape(rows * cols, ch), w, preferred_element_type=jnp.float32).reshape(rows, cols, ch)


def call(kernel, out_shape, scratch, args, flops, any_args=()):
    return pl.pallas_call(
        kernel,
        out_shape=out_shape,
        in_specs=[
            pl.BlockSpec(memory_space=pl.ANY) if k in any_args else pl.BlockSpec(memory_space=pltpu.VMEM)
            for k in range(len(args))
        ],
        out_specs=jax.tree.map(lambda _: pl.BlockSpec(memory_space=pltpu.VMEM), out_shape),
        scratch_shapes=scratch,
        compiler_params=pltpu.CompilerParams(vmem_limit_bytes=VMEM_LIMIT),
        cost_estimate=pl.CostEstimate(flops=int(flops), transcendentals=0, bytes_accessed=0),
    )(*args)


def taps_sent(plan, col):
    return (2 * col,) if plan.two else (0, 2)


def taps_got(plan, col):
    return (2 - 2 * col,) if plan.two else (0, 2)


def far_rows(plan):
    group = lax.axis_index("row") // (FAR // plan.tile_rows)
    one = 2 - 2 * (group % 2)
    return one, 2 - one


def far_one(plan, a, b, w, stream, part_one, part_two, own_a, own_b, *side_b):
    col = lax.axis_index("col")
    one, two = far_rows(plan)
    half = a.shape[0]
    part_one[...] = times(a[...], w[two, 1])
    part_two[...] = times(a[...], w[one, 1])
    own_a[...] = stream[0:half] + times(a[...], w[1, 1])
    own_b[...] = stream[half : 2 * half] + times(b[...], w[1, 1])
    for ref, tap in zip(side_b, taps_sent(plan, col)):
        ref[...] = times(b[...], w[1, tap])


def far_two(plan, n_side, *refs):
    crossed = refs[:n_side]
    got_one, got_two, w, part_one, part_two = refs[n_side : n_side + 5]
    side_b = refs[n_side + 5 : 2 * n_side + 5]
    out_one, out_two = refs[2 * n_side + 5 : 2 * n_side + 7]
    side_out = refs[2 * n_side + 7 :]
    col = lax.axis_index("col")
    one, two = far_rows(plan)
    for part, out, tap_row in ((part_one, out_one, two), (part_two, out_two, one)):
        total = part[...]
        for ref, tap in zip(crossed, taps_got(plan, col)):
            total = total + times(ref[...], w[tap_row, tap])
        out[...] = total.astype(out.dtype)
    for ref, acc, tap in zip(side_out, side_b, taps_sent(plan, col)):
        ref[...] = (acc[...] + times(got_one[...], w[one, tap]) + times(got_two[...], w[two, tap])).astype(ref.dtype)


def far_three(plan, n_side, *refs):
    crossed = refs[:n_side]
    got_one, got_two, w, own_a, own_b, out_a, out_b = refs[n_side:]
    col = lax.axis_index("col")
    one, two = far_rows(plan)
    total = own_a[...]
    for ref, tap in zip(crossed, taps_got(plan, col)):
        total = total + times(ref[...], w[1, tap])
    out_a[...] = total
    out_b[...] = own_b[...] + times(got_one[...], w[one, 1]) + times(got_two[...], w[two, 1])


def far_four(n_side, own_a, own_b, from_above, from_below, *refs):
    side_b, (out_ref,) = refs[:n_side], refs[n_side:]
    half = own_a.shape[0]
    out_ref[0:half] = own_a[...] + from_above[...].astype(jnp.float32) + from_below[...].astype(jnp.float32)
    total = own_b[...]
    for ref in side_b:
        total = total + ref[...].astype(jnp.float32)
    out_ref[half : 2 * half] = total


def pair(value, hop, parity):
    n_row, n_col = lax.axis_size("row"), lax.axis_size("col")
    ups = [
        (r * n_col + c, (r + hop) * n_col + c)
        for r in range(n_row - hop)
        for c in range(n_col)
        if r // hop % 2 == parity
    ]
    return lax.ppermute(value, ("row", "col"), ups + [(j, i) for i, j in ups])


def move(value, rows, cols):
    n_row, n_col = lax.axis_size("row"), lax.axis_size("col")
    pairs = [
        (r * n_col + c, (r + rows) * n_col + c + cols)
        for r in range(n_row)
        for c in range(n_col)
        if 0 <= r + rows < n_row and 0 <= c + cols < n_col
    ]
    return lax.ppermute(value, ("row", "col"), pairs)


def cross(value):
    return lax.ppermute(value, "col", [(0, 1), (1, 0)])


def local(features, inner_weights, far_weights, gains):
    tile_rows, tile_cols, ch = features.shape
    plan = Plan(tile_rows, tile_cols, ch, lax.axis_size("row"), lax.axis_size("col"))
    col = lax.axis_index("col")
    d_one, d_two, d_three, d_four = DILATIONS
    halo = d_one + d_two
    ext, width, width4 = plan.ext, plan.width, plan.width4
    bf16, f32 = jnp.bfloat16, jnp.float32
    shape, vmem, dma = jax.ShapeDtypeStruct, pltpu.VMEM, pltpu.SemaphoreType.DMA
    weights = inner_weights.reshape(inner_weights.shape[0], 9 * ch, ch)
    if plan.two:
        edge = lax.dynamic_slice_in_dim(features, (1 - col) * (tile_cols - ext), ext, axis=1)
        sides = [cross(edge)]
    else:
        sides = [move(features[:, tile_cols - ext :], 0, 1), move(features[:, :ext], 0, -1)]
    n_side = len(sides)
    halo_shape = shape((halo, width, ch), bf16)
    one, two = call(
        functools.partial(gather_rows, plan, halo),
        (halo_shape, halo_shape),
        [dma((2 * (1 + n_side),))],
        (features, *sides),
        1,
    )
    got_two, got_one = pair(two, 1, 1), pair(one, 1, 0)
    per_row = 2 * 9 * ch * ch
    whole = 9 * ch
    n_mid = tile_rows - 2 * d_two
    line = vmem((tile_rows, width + 2 * PAD, ch), f32)
    taps = vmem((tile_rows, width, 3 * ch), bf16)
    mid, mid_act, edge_act, edge_base = call(
        functools.partial(one_own, plan, halo),
        (
            shape((n_mid, width, ch), f32),
            shape((n_mid, width, ch), bf16),
            shape((2 * halo, width, ch), bf16),
            shape((2 * halo, width, ch), f32),
        ),
        [vmem((tile_rows, width, ch), f32), line, taps, vmem((whole, ch), bf16), dma],
        (features, *sides, weights, gains),
        per_row * n_mid * width,
        any_args=(1 + n_side,),
    )
    sent = shape((d_three, width, ch), bf16)
    stream2, act3, one, two = call(
        functools.partial(one_two, plan, halo),
        (shape((tile_rows, width, ch), f32), shape((tile_rows, width, ch), bf16), sent, sent),
        [
            vmem((4 * halo, width, ch), f32),
            vmem((n_mid + 2 * CHUNK, width + 2 * PAD, ch), f32),
            vmem((4 * halo, width, 3 * ch), bf16),
            vmem((2 * CHUNK, width, ch), f32),
            vmem((n_mid + 2 * CHUNK, width, 3 * ch), bf16),
            vmem((whole, ch), bf16),
            vmem((whole, ch), bf16),
            dma((2,)),
        ],
        (got_one, got_two, mid, mid_act, edge_act, edge_base, weights, gains),
        per_row * (2 * CHUNK + tile_rows) * width,
        any_args=(6,),
    )
    got_two, got_one = pair(two, 1, 1), pair(one, 1, 0)
    n_mid = tile_rows - 2 * d_three
    row_f32 = vmem((tile_rows, width, ch), f32)
    edge, mid, mid_act = call(
        functools.partial(three_own, plan),
        (
            shape((2 * d_three, width, ch), f32),
            shape((n_mid, tile_cols, ch), f32),
            shape((n_mid, width4, ch), bf16),
        ),
        [line, taps, row_f32, row_f32, vmem((whole, ch), bf16), dma],
        (act3, weights, stream2, gains),
        per_row * tile_rows * width,
        any_args=(1,),
    )
    sent = shape((d_four, width4, ch), bf16)
    stream3, act4, one, two = call(
        functools.partial(three_rim, plan),
        (shape((tile_rows, tile_cols, ch), f32), shape((tile_rows, width4, ch), bf16), sent, sent),
        [
            vmem((2 * d_three, width + 2 * PAD, ch), f32),
            vmem((2 * d_three, width, 3 * ch), bf16),
            vmem((2, 3 * ch, ch), bf16),
            vmem((2 * d_three, width, ch), f32),
            vmem((2 * d_three, width, ch), f32),
            dma((2,)),
        ],
        (got_one, got_two, edge, mid, mid_act, weights, gains),
        per_row * 2 * d_three * width / 3,
        any_args=(5,),
    )
    got_two, got_one = pair(two, 1, 1), pair(one, 1, 0)
    line = vmem((tile_rows, width4 + 2 * PAD, ch), f32)
    taps = vmem((tile_rows, tile_cols, 3 * ch), bf16)
    acc4 = call(
        functools.partial(four_own, plan),
        shape((tile_rows, tile_cols, ch), f32),
        [line, taps, vmem((whole, ch), bf16), dma],
        (act4, weights, stream3),
        per_row * tile_rows * tile_cols,
        any_args=(1,),
    )
    half = tile_rows // 2
    stream4, a, b = call(
        functools.partial(four_rim, plan),
        (
            shape((tile_rows, tile_cols, ch), f32),
            shape((half, tile_cols, ch), bf16),
            shape((half, tile_cols, ch), bf16),
        ),
        [line, taps, vmem((2, 3 * ch, ch), bf16), dma((2,))],
        (got_one, got_two, acc4, weights, gains),
        per_row * 2 * d_four * tile_cols / 3,
        any_args=(3,),
    )
    row_hop, col_hop = FAR // tile_rows, FAR // tile_cols
    if plan.two:
        crossed = [cross(a)]
    else:
        crossed = [move(a, 0, col_hop), move(a, 0, -col_hop)]
    got_one, got_two = pair(b, row_hop, 0), pair(b, row_hop, 1)
    block = shape((half, tile_cols, ch), f32)
    sent = shape((half, tile_cols, ch), bf16)
    per_half = 2 * ch * ch * half * tile_cols
    part_one, part_two, own_a, own_b, *side_b = call(
        functools.partial(far_one, plan),
        [block] * (4 + n_side),
        [],
        (a, b, far_weights, stream4),
        per_half * 5,
    )
    one, two, *sides = call(
        functools.partial(far_two, plan, n_side),
        [sent] * (2 + n_side),
        [],
        (*crossed, got_one, got_two, far_weights, part_one, part_two, *side_b),
        per_half * 4,
    )
    back_one, back_two = pair(one, row_hop, 0), pair(two, row_hop, 1)
    if plan.two:
        side_got = [cross(sides[0])]
    else:
        side_got = [move(sides[0], 0, col_hop), move(sides[1], 0, -col_hop)]
    own_a, own_b = call(
        functools.partial(far_three, plan, n_side),
        [block] * 2,
        [],
        (*crossed, got_one, got_two, far_weights, own_a, own_b),
        per_half * 3,
    )
    return call(
        functools.partial(far_four, n_side),
        shape((tile_rows, tile_cols, ch), f32),
        [],
        (own_a, own_b, back_one, back_two, *side_got),
        1,
    )


def solution(mesh):
    return jax.shard_map(
        local,
        mesh=mesh,
        in_specs=(P("row", "col", None), P(), P(), P()),
        out_specs=P("row", "col", None),
        check_vma=False,
    )
```

```python
import functools

import jax
import jax.numpy as jnp
from jax import lax
from jax.experimental import pallas as pl
from jax.experimental.pallas import tpu as pltpu
from jax.sharding import PartitionSpec as P

FAR = 64
DILATIONS = (1, 2, 4, 8)
PAD = 8
VMEM_LIMIT = 20 * 1024 * 1024


def normed(stream, gain):
    centre = jnp.mean(stream, axis=-1, keepdims=True)
    moved = stream - centre
    spread = jnp.mean(moved * moved, axis=-1, keepdims=True)
    return jax.nn.gelu(moved * lax.rsqrt(spread + 1e-05) * gain)


def spread_taps(line_ref, taps_ref, row, dilation, start, cols):
    ch = line_ref.shape[-1]
    for tap in range(3):
        shift = (tap - 1) * dilation
        taps_ref[row, :, tap * ch : (tap + 1) * ch] = line_ref[row, pl.ds(start + shift, cols), :].astype(
            taps_ref.dtype
        )


def clear_edges(line_ref):
    rows, width, ch = line_ref.shape
    line_ref[:, 0:PAD, :] = jnp.zeros((rows, PAD, ch), line_ref.dtype)
    line_ref[:, width - PAD : width, :] = jnp.zeros((rows, PAD, ch), line_ref.dtype)


def conv_part(taps_ref, weight_ref, first, rows, dilation, taps=(0, 1, 2)):
    cols, depth = taps_ref.shape[1:]
    lhs = [taps_ref[first + tap * dilation : first + tap * dilation + rows].reshape(rows * cols, depth) for tap in taps]
    lhs = lhs[0] if len(lhs) == 1 else jnp.concatenate(lhs, axis=1)
    weight = weight_ref[taps[0] * depth : (taps[-1] + 1) * depth, :]
    out = jnp.dot(lhs, weight, preferred_element_type=jnp.float32)
    return out.reshape(rows, cols, out.shape[-1])


def in_grid(col_lo, col_hi, value):
    cols = lax.broadcasted_iota(jnp.int32, value.shape, 0)
    keep = (cols >= col_lo) & (cols < col_hi)
    return jnp.where(keep, value, 0.0)


class Plan:
    def __init__(self, tile_rows, tile_cols, ch, n_row, n_col):
        self.tile_rows, self.tile_cols, self.ch = tile_rows, tile_cols, ch
        self.n_row, self.n_col = n_row, n_col
        self.two = n_col == 2
        self.ext = -(-sum(DILATIONS) // 16) * 16
        self.width = tile_cols + (self.ext if self.two else 2 * self.ext)
        self.last = DILATIONS[-1]
        self.width4 = tile_cols + (self.last if self.two else 2 * self.last)

    def own(self, col):
        return pl.multiple_of(col * self.ext, 8) if self.two else self.ext

    def own4(self, col):
        return pl.multiple_of(col * self.last, 8) if self.two else self.last

    def start4(self, col):
        return pl.multiple_of(col * (self.ext - self.last), 8) if self.two else self.ext - self.last

    def sides(self, col):
        if self.two:
            return (pl.multiple_of((1 - col) * self.tile_cols, 8),)
        return (0, self.ext + self.tile_cols)

    def edges(self, col):
        if self.two:
            return (pl.multiple_of((1 - col) * (self.tile_cols - self.ext), 16),)
        return self.tile_cols - self.ext, 0

    def col_range(self, col):
        if self.two:
            return 0, self.width
        lo = jnp.where(col == 0, self.ext, 0)
        hi = jnp.where(col == self.n_col - 1, self.ext + self.tile_cols, self.width)
        return lo, hi

    def inside(self, col, value):
        if self.two:
            return value
        return in_grid(*self.col_range(col), value)

    def starts(self, row_id, span):
        last = self.tile_rows - span
        one = jnp.where(row_id % 2 == 0, last, 0)
        return one, last - one


def lay(line, taps, row, value, dilation, start, cols):
    width = value.shape[0]
    line[row, PAD : PAD + width, :] = value
    spread_taps(line, taps, row, dilation, start, cols)


def rows_of(count, body, step=4):
    def block(k, _):
        for j in range(step):
            body(k * step + j)
        return 0

    lax.fori_loop(0, count // step, block, 0)
    for row in range(count // step * step, count):
        body(row)


def stage(plan, halo, features, gains, *refs):
    n_side = 1 if plan.two else 2
    tile, gains_out = refs[:2]
    edges, outs, (sems,) = refs[2 : 2 + n_side], refs[2 + n_side : 4 + n_side], refs[4 + n_side :]
    row_id, col = lax.axis_index("row"), lax.axis_index("col")
    moves = [(features.at[:, pl.ds(at, plan.ext)], edge) for at, edge in zip(plan.edges(col), edges)]
    moves += [(features.at[pl.ds(at, halo)], out) for at, out in zip(plan.starts(row_id, halo), outs)]
    moves += [(gains, gains_out), (features, tile)]
    copies = [pltpu.make_async_copy(src, dst, sems.at[k]) for k, (src, dst) in enumerate(moves)]
    for copy in copies:
        copy.start()
    for copy in copies:
        copy.wait()


def corners(plan, one, two, after, *refs):
    del after
    outs, (sems,) = refs[:-1], refs[-1:]
    col = lax.axis_index("col")
    halo = one.shape[0]
    copies = []
    for out, at in zip(outs, plan.edges(col)):
        for k, ref in enumerate((one, two)):
            copies.append(
                pltpu.make_async_copy(
                    ref.at[:, pl.ds(at, plan.ext)], out.at[pl.ds(k * halo, halo)], sems.at[len(copies)]
                )
            )
    for copy in copies:
        copy.start()
    for copy in copies:
        copy.wait()


CHUNK = 4


def one_prepare(plan, halo, *refs):
    n_side = 1 if plan.two else 2
    parts = refs[: 1 + n_side]
    gains, w_hbm, base, taps, w_one, line, sem = refs[1 + n_side :]
    copy = fetch(w_hbm, 0, w_one, sem)
    copy.start()
    col = lax.axis_index("col")
    for part, offset in zip(parts, (plan.own(col),) + plan.sides(col)):
        base[:, pl.ds(offset, part.shape[1]), :] = part[...].astype(jnp.float32)
    clear_edges(line)

    def prepare(row):
        lay(line, taps, row, plan.inside(col, normed(base[row], gains[0:1, :])), DILATIONS[0], PAD, plan.width)

    rows_of(plan.tile_rows, prepare)
    copy.wait()


def fetch(w_hbm, layer, out, sem):
    return pltpu.make_async_copy(w_hbm.at[layer], out, sem)


def one_own(plan, halo, base, taps, w_one, w_hbm, gains, mid, mid_act, w_next, sem):
    col = lax.axis_index("col")
    copy = fetch(w_hbm, 1, w_next, sem)
    copy.start()

    def follow(row):
        mid_act[row] = plan.inside(col, normed(mid[row], gains[1:2, :])).astype(mid_act.dtype)

    edge = DILATIONS[1]
    count = mid.shape[0] // CHUNK
    for k in range(count):
        at = k * CHUNK
        mid[at : at + CHUNK] = base[edge + at : edge + at + CHUNK] + conv_part(
            taps, w_one, edge + at - DILATIONS[0], CHUNK, DILATIONS[0]
        )
        if k:
            for row in range(at - CHUNK, at):
                follow(row)
    rows_of(CHUNK, lambda row: follow((count - 1) * CHUNK + row))
    copy.wait()


def one_two(plan, halo, *refs):
    n_side = 1 if plan.two else 2
    got, crossed, refs = refs[:2], refs[2 : 2 + n_side], refs[2 + n_side :]
    mid, mid_act, own_taps, own_base, w_one, w_two, w_hbm, gains = refs[:8]
    stream, taps_out, send_one, send_two, w_next = refs[8:13]
    base, line, taps_one, rim, taps_two, sem = refs[13:]
    line_out = line
    row_id, col = lax.axis_index("row"), lax.axis_index("col")
    copy = fetch(w_hbm, 2, w_next, sem)
    copy.start()
    rows, width, ch = plan.tile_rows, plan.width, plan.ch
    d_one, d_two = DILATIONS[:2]
    clear_edges(line)
    for k, first in enumerate((0, rows - halo)):
        at = (k + 1) * halo
        base[at : at + halo] = own_base[first : first + halo]
        taps_one[at : at + halo] = own_taps[first : first + halo]
    top = (halo * 3) * (1 - row_id % 2)
    for k, (ref, at) in enumerate(zip(got, (top, 3 * halo - top))):
        base[pl.ds(at, halo), pl.ds(plan.own(col), ref.shape[1]), :] = ref[...].astype(jnp.float32)
        for side, offset in zip(crossed, plan.sides(col)):
            base[pl.ds(at, halo), pl.ds(offset, side.shape[1]), :] = side[k * halo : (k + 1) * halo].astype(jnp.float32)
    for row in tuple(range(halo)) + tuple(range(3 * halo, 4 * halo)):
        lay(line, taps_one, row, plan.inside(col, normed(base[row], gains[0:1, :])), d_one, PAD, width)
    n_mid = mid.shape[0]

    def spread_mid(row):
        lay(line, taps_two, 2 * d_two + row, mid_act[row].astype(jnp.float32), d_two, PAD, width)

    for k in range(2):
        at = 2 * halo * k
        rim[k * CHUNK : (k + 1) * CHUNK] = base[at + 1 : at + 1 + CHUNK] + conv_part(taps_one, w_one, at, CHUNK, d_one)
        for row in range(k * n_mid // 2, (k + 1) * n_mid // 2):
            spread_mid(row)

    def spread_rim(row):
        value = plan.inside(col, normed(rim[row], gains[1:2, :]))
        if row < d_two:
            value = jnp.where(row_id == 0, 0.0, value)
        if row >= 2 * CHUNK - d_two:
            value = jnp.where(row_id == plan.n_row - 1, 0.0, value)
        lay(line, taps_two, row if row < CHUNK else n_mid + row, value, d_two, PAD, width)

    def finish(row):
        lay(line_out, taps_out, row, plan.inside(col, normed(stream[row], gains[2:3, :])), DILATIONS[2], PAD, width)

    def second(first):
        return conv_part(taps_two, w_two, first, CHUNK, d_two)

    inner = tuple(range(CHUNK, rows - CHUNK, CHUNK))
    per = -(-2 * CHUNK // len(inner))
    for k, first in enumerate(inner):
        stream[first : first + CHUNK] = mid[first - d_two : first - d_two + CHUNK] + second(first)
        for row in range(k * per, min((k + 1) * per, 2 * CHUNK)):
            spread_rim(row)
    out = second(0)
    stream[0:d_two] = rim[d_two : 2 * d_two] + out[:d_two]
    stream[d_two:CHUNK] = mid[0 : CHUNK - d_two] + out[d_two:]
    for first in inner[: len(inner) // 2]:
        for row in range(first, first + CHUNK):
            finish(row)
    last = rows - CHUNK
    out = second(last)
    stream[last : last + d_two] = mid[n_mid - d_two : n_mid] + out[:d_two]
    stream[last + d_two : rows] = rim[CHUNK : CHUNK + d_two] + out[d_two:]
    for first in inner[len(inner) // 2 :]:
        for row in range(first, first + CHUNK):
            finish(row)
    rows_of(CHUNK, finish)
    rows_of(CHUNK, lambda row: finish(last + row))
    for ref, at in zip((send_one, send_two), plan.starts(row_id, DILATIONS[2])):
        ref[...] = taps_out[pl.ds(at, DILATIONS[2]), :, ch : 2 * ch]
    copy.wait()


def three_own(plan, taps, weight, w_hbm, stream, gains, edge, mid, mid_act, w_next, full, row_act, sem):
    col = lax.axis_index("col")
    copy = fetch(w_hbm, 3, w_next, sem)
    copy.start()
    d = DILATIONS[2]
    rows = plan.tile_rows
    for first in range(d, rows - d, CHUNK):
        full[first - d : first - d + CHUNK] = stream[first : first + CHUNK] + conv_part(taps, weight, first - d, CHUNK, d)

    def finish(row):
        emit(plan, col, full, row_act, row, gains[3:4, :], mid, mid_act, row)

    count = rows - 2 * d
    edge[0:d] = stream[0:d] + conv_part(taps, weight, -d, d, d, (1, 2))
    for row in range(count // 2):
        finish(row)
    edge[d : 2 * d] = stream[rows - d : rows] + conv_part(taps, weight, rows - 2 * d, d, d, (0, 1))
    for row in range(count // 2, count):
        finish(row)
    copy.wait()


def emit(plan, col, full, row_act, row, gain, stream, act, at):
    row_act[row] = plan.inside(col, normed(full[row], gain))
    act[at] = row_act[row, pl.ds(plan.start4(col), plan.width4), :].astype(act.dtype)
    stream[at] = full[row, pl.ds(plan.own(col), plan.tile_cols), :]


def partner_weight(plan, row_id, k, weight):
    depth = 3 * plan.ch
    one = jnp.where(row_id % 2 == 0, 2 * depth, 0)
    return weight.at[pl.ds(pl.multiple_of((one, 2 * depth - one)[k], 128), depth)]


def three_rim(plan, got_one, got_two, edge, mid, mid_act, weight, gains, stream, act, send_one, send_two, *scratch):
    line, taps, full, row_act = scratch
    row_id, col = lax.axis_index("row"), lax.axis_index("col")
    d = DILATIONS[2]
    rows, width = plan.tile_rows, plan.width
    clear_edges(line)
    for k, ref in enumerate((got_one, got_two)):
        for row in range(d):
            lay(line, taps, k * d + row, ref[row].astype(jnp.float32), d, PAD, width)
    stream[d : rows - d] = mid[...]
    act[d : rows - d] = mid_act[...]
    at_one, at_two = plan.starts(row_id, d)
    half = jnp.where(row_id % 2 == 0, d, 0)
    for k, (place, at) in enumerate(((half, at_one), (d - half, at_two))):
        full[k * d : (k + 1) * d] = edge[pl.ds(place, d)] + conv_part(
            taps, partner_weight(plan, row_id, k, weight), k * d, d, d, (0,)
        )
    for k, at in enumerate((at_one, at_two)):
        for row in range(d):
            emit(plan, col, full, row_act, k * d + row, gains[3:4, :], stream, act, at + row)
    for ref, at in zip((send_one, send_two), plan.starts(row_id, DILATIONS[3])):
        ref[...] = act[pl.ds(at, DILATIONS[3])]


def four_own(plan, act, weight, stream, out, line, taps):
    col = lax.axis_index("col")
    d = DILATIONS[3]
    rows, cols = plan.tile_rows, plan.tile_cols
    start = PAD + plan.own4(col)
    clear_edges(line)
    rows_of(rows, lambda row: lay(line, taps, row, act[row].astype(jnp.float32), d, start, cols))
    for first in range(0, rows, CHUNK):
        used = tuple(t for t in range(3) if 0 <= first + (t - 1) * d < rows)
        out[first : first + CHUNK] = stream[first : first + CHUNK] + conv_part(taps, weight, first - d, CHUNK, d, used)


def four_rim(plan, k, got, acc, weight, gains, stream, act, line, taps):
    row_id, col = lax.axis_index("row"), lax.axis_index("col")
    d = DILATIONS[3]
    start = PAD + plan.own4(col)
    clear_edges(line)

    def spread(row):
        lay(line, taps, row, got[row].astype(jnp.float32), d, start, plan.tile_cols)

    def finish(row):
        act[row] = normed(stream[row], gains[4:5, :]).astype(act.dtype)

    for row in range(CHUNK):
        spread(row)
    at = plan.starts(row_id, d)[k]
    for first in range(0, d, CHUNK):
        stream[first : first + CHUNK] = acc[pl.ds(at + first, CHUNK)] + conv_part(
            taps, partner_weight(plan, row_id, k, weight), first, CHUNK, d, (0,)
        )
        if first:
            for row in range(first - CHUNK, first):
                finish(row)
        for row in range(first + CHUNK, min(first + 2 * CHUNK, d)):
            spread(row)
    for row in range(d - CHUNK, d):
        finish(row)


def times(a, w):
    rows, cols, ch = a.shape
    return jnp.dot(a.reshape(rows * cols, ch), w, preferred_element_type=jnp.float32).reshape(rows, cols, ch)


def call(kernel, out_shape, scratch, args, flops, any_args=()):
    return pl.pallas_call(
        kernel,
        out_shape=out_shape,
        in_specs=[
            pl.BlockSpec(memory_space=pltpu.HBM) if k in any_args else pl.BlockSpec(memory_space=pltpu.VMEM)
            for k in range(len(args))
        ],
        out_specs=jax.tree.map(lambda _: pl.BlockSpec(memory_space=pltpu.VMEM), out_shape),
        scratch_shapes=scratch,
        compiler_params=pltpu.CompilerParams(vmem_limit_bytes=VMEM_LIMIT),
        cost_estimate=pl.CostEstimate(flops=int(flops), transcendentals=0, bytes_accessed=0),
    )(*args)


def taps_sent(plan, col):
    return (2 * col,) if plan.two else (0, 2)


def taps_got(plan, col):
    return (2 - 2 * col,) if plan.two else (0, 2)


def far_rows(plan):
    group = lax.axis_index("row") // (FAR // plan.tile_rows)
    one = 2 - 2 * (group % 2)
    return one, 2 - one


def far_a(plan, a, w, stream, part_one, part_two, own):
    one, two = far_rows(plan)
    part_one[...] = times(a[...], w[two, 1])
    part_two[...] = times(a[...], w[one, 1])
    own[...] = stream[...] + times(a[...], w[1, 1])


def far_b(plan, b, w, stream, own, *side):
    col = lax.axis_index("col")
    own[...] = stream[...] + times(b[...], w[1, 1])
    for ref, tap in zip(side, taps_sent(plan, col)):
        ref[...] = times(b[...], w[1, tap])


def far_two(plan, n_side, *refs):
    crossed = refs[:n_side]
    got_one, got_two, w, part_one, part_two = refs[n_side : n_side + 5]
    side_b = refs[n_side + 5 : 2 * n_side + 5]
    out_one, out_two = refs[2 * n_side + 5 : 2 * n_side + 7]
    side_out = refs[2 * n_side + 7 :]
    col = lax.axis_index("col")
    one, two = far_rows(plan)
    for part, out, tap_row in ((part_one, out_one, two), (part_two, out_two, one)):
        total = part[...]
        for ref, tap in zip(crossed, taps_got(plan, col)):
            total = total + times(ref[...], w[tap_row, tap])
        out[...] = total.astype(out.dtype)
    for ref, acc, tap in zip(side_out, side_b, taps_sent(plan, col)):
        ref[...] = (acc[...] + times(got_one[...], w[one, tap]) + times(got_two[...], w[two, tap])).astype(ref.dtype)


def far_three(plan, n_side, *refs):
    crossed = refs[:n_side]
    got_one, got_two, w, own_a, own_b, out_a, out_b = refs[n_side:]
    col = lax.axis_index("col")
    one, two = far_rows(plan)
    total = own_a[...]
    for ref, tap in zip(crossed, taps_got(plan, col)):
        total = total + times(ref[...], w[1, tap])
    out_a[...] = total
    out_b[...] = own_b[...] + times(got_one[...], w[one, 1]) + times(got_two[...], w[two, 1])


def far_four(plan, n_side, own_a, own_b, back_one, back_two, *refs):
    side_b, (out_ref,) = refs[:n_side], refs[n_side:]
    half = own_a.shape[0]
    at_a, at_b = plan.starts(lax.axis_index("row"), half)
    out_ref[pl.ds(at_a, half)] = own_a[...] + back_one[...].astype(jnp.float32) + back_two[...].astype(jnp.float32)
    total = own_b[...]
    for ref in side_b:
        total = total + ref[...].astype(jnp.float32)
    out_ref[pl.ds(at_b, half)] = total


def pair(value, hop, parity):
    n_row, n_col = lax.axis_size("row"), lax.axis_size("col")
    ups = [
        (r * n_col + c, (r + hop) * n_col + c)
        for r in range(n_row - hop)
        for c in range(n_col)
        if r // hop % 2 == parity
    ]
    return lax.ppermute(value, ("row", "col"), ups + [(j, i) for i, j in ups])


def move(value, rows, cols):
    n_row, n_col = lax.axis_size("row"), lax.axis_size("col")
    pairs = [
        (r * n_col + c, (r + rows) * n_col + c + cols)
        for r in range(n_row)
        for c in range(n_col)
        if 0 <= r + rows < n_row and 0 <= c + cols < n_col
    ]
    return lax.ppermute(value, ("row", "col"), pairs)


def cross(value):
    return lax.ppermute(value, "col", [(0, 1), (1, 0)])


def local(features, inner_weights, far_weights, gains):
    tile_rows, tile_cols, ch = features.shape
    plan = Plan(tile_rows, tile_cols, ch, lax.axis_size("row"), lax.axis_size("col"))
    col = lax.axis_index("col")
    d_one, d_two, d_three, d_four = DILATIONS
    halo = d_one + d_two
    ext, width, width4 = plan.ext, plan.width, plan.width4
    bf16, f32 = jnp.bfloat16, jnp.float32
    shape, vmem, dma = jax.ShapeDtypeStruct, pltpu.VMEM, pltpu.SemaphoreType.DMA
    weights = pltpu.with_memory_space_constraint(inner_weights.reshape(inner_weights.shape[0], 9 * ch, ch), pltpu.HBM)
    n_side = 1 if plan.two else 2
    halo_shape, edge_shape = shape((halo, tile_cols, ch), bf16), shape((tile_rows, ext, ch), bf16)
    tile, gains, *refs = call(
        functools.partial(stage, plan, halo),
        [shape(features.shape, bf16), shape(gains.shape, f32)] + [edge_shape] * n_side + [halo_shape] * 2,
        [dma((4 + n_side,))],
        tuple(pltpu.with_memory_space_constraint(value, pltpu.HBM) for value in (features, gains)),
        1,
        any_args=(0, 1),
    )
    edges, (one, two) = refs[:n_side], refs[n_side:]

    def spread_sides(values):
        if plan.two:
            return [cross(values[0])]
        return [move(values[0], 0, 1), move(values[1], 0, -1)]

    sides = spread_sides(edges)
    got_two, got_one = pair(two, 1, 1), pair(one, 1, 0)
    per_row = 2 * 9 * ch * ch
    whole = 9 * ch
    n_mid = tile_rows - 2 * d_two
    line = vmem((tile_rows, width + 2 * PAD, ch), f32)
    taps = vmem((tile_rows, width, 3 * ch), bf16)
    w_shape = shape((whole, ch), bf16)
    base, taps1, w_one = call(
        functools.partial(one_prepare, plan, halo),
        (shape((tile_rows, width, ch), f32), shape((tile_rows, width, 3 * ch), bf16), w_shape),
        [line, dma],
        (tile, *sides, gains, weights),
        per_row * 8 * width,
        any_args=(2 + n_side,),
    )
    crossed = spread_sides(
        call(
            functools.partial(corners, plan),
            [shape((2 * halo, ext, ch), bf16)] * n_side,
            [dma((2 * n_side,))],
            (got_one, got_two, taps1),
            1,
            any_args=(2,),
        )
    )
    mid, mid_act, w_two = call(
        functools.partial(one_own, plan, halo),
        (shape((n_mid, width, ch), f32), shape((n_mid, width, ch), bf16), w_shape),
        [dma],
        (base, taps1, w_one, weights, gains),
        per_row * n_mid * width,
        any_args=(3,),
    )
    sent = shape((d_three, width, ch), bf16)
    stream2, taps3, one, two, w_three = call(
        functools.partial(one_two, plan, halo),
        (shape((tile_rows, width, ch), f32), shape((tile_rows, width, 3 * ch), bf16), sent, sent, w_shape),
        [
            vmem((4 * halo, width, ch), f32),
            vmem((n_mid + 2 * CHUNK, width + 2 * PAD, ch), f32),
            vmem((4 * halo, width, 3 * ch), bf16),
            vmem((2 * CHUNK, width, ch), f32),
            vmem((n_mid + 2 * CHUNK, width, 3 * ch), bf16),
            dma,
        ],
        (got_one, got_two, *crossed, mid, mid_act, taps1, base, w_one, w_two, weights, gains),
        per_row * (2 * CHUNK + tile_rows) * width,
        any_args=(8 + n_side,),
    )
    got_two, got_one = pair(two, 1, 1), pair(one, 1, 0)
    n_mid = tile_rows - 2 * d_three
    row_f32 = vmem((tile_rows, width, ch), f32)
    edge, mid, mid_act, w_four = call(
        functools.partial(three_own, plan),
        (
            shape((2 * d_three, width, ch), f32),
            shape((n_mid, tile_cols, ch), f32),
            shape((n_mid, width4, ch), bf16),
            w_shape,
        ),
        [row_f32, row_f32, dma],
        (taps3, w_three, weights, stream2, gains),
        per_row * tile_rows * width,
        any_args=(2,),
    )
    sent = shape((d_four, width4, ch), bf16)
    stream3, act4, one, two = call(
        functools.partial(three_rim, plan),
        (shape((tile_rows, tile_cols, ch), f32), shape((tile_rows, width4, ch), bf16), sent, sent),
        [
            vmem((2 * d_three, width + 2 * PAD, ch), f32),
            vmem((2 * d_three, width, 3 * ch), bf16),
            vmem((2 * d_three, width, ch), f32),
            vmem((2 * d_three, width, ch), f32),
        ],
        (got_one, got_two, edge, mid, mid_act, w_three, gains),
        per_row * 2 * d_three * width / 3,
    )
    got_two, got_one = pair(two, 1, 1), pair(one, 1, 0)
    line = vmem((tile_rows, width4 + 2 * PAD, ch), f32)
    taps = vmem((tile_rows, tile_cols, 3 * ch), bf16)
    acc4 = call(
        functools.partial(four_own, plan),
        shape((tile_rows, tile_cols, ch), f32),
        [line, taps],
        (act4, w_four, stream3),
        per_row * tile_rows * tile_cols,
    )
    half = tile_rows // 2
    if half != d_four or FAR // tile_rows % 2:
        raise ValueError("tile rows")
    finished = [
        call(
            functools.partial(four_rim, plan, k),
            (shape((half, tile_cols, ch), f32), shape((half, tile_cols, ch), bf16)),
            [
                vmem((d_four, width4 + 2 * PAD, ch), f32),
                vmem((d_four, tile_cols, 3 * ch), bf16),
            ],
            (got, acc4, w_four, gains),
            per_row * d_four * tile_cols / 3,
        )
        for k, got in enumerate((got_one, got_two))
    ]
    (stream_a, a), (stream_b, b) = finished
    row_hop, col_hop = FAR // tile_rows, FAR // tile_cols
    if plan.two:
        crossed = [cross(a)]
    else:
        crossed = [move(a, 0, col_hop), move(a, 0, -col_hop)]
    got_one, got_two = pair(b, row_hop, 0), pair(b, row_hop, 1)
    block = shape((half, tile_cols, ch), f32)
    sent = shape((half, tile_cols, ch), bf16)
    per_half = 2 * ch * ch * half * tile_cols
    part_one, part_two, own_a = call(
        functools.partial(far_a, plan), [block] * 3, [], (a, far_weights, stream_a), per_half * 3
    )
    own_b, *side_b = call(
        functools.partial(far_b, plan), [block] * (1 + n_side), [], (b, far_weights, stream_b), per_half * 2
    )
    one, two, *sides = call(
        functools.partial(far_two, plan, n_side),
        [sent] * (2 + n_side),
        [],
        (*crossed, got_one, got_two, far_weights, part_one, part_two, *side_b),
        per_half * 4,
    )
    back_one, back_two = pair(one, row_hop, 0), pair(two, row_hop, 1)
    if plan.two:
        side_got = [cross(sides[0])]
    else:
        side_got = [move(sides[0], 0, col_hop), move(sides[1], 0, -col_hop)]
    own_a, own_b = call(
        functools.partial(far_three, plan, n_side),
        [block] * 2,
        [],
        (*crossed, got_one, got_two, far_weights, own_a, own_b),
        per_half * 3,
    )
    return call(
        functools.partial(far_four, plan, n_side),
        shape((tile_rows, tile_cols, ch), f32),
        [],
        (own_a, own_b, back_one, back_two, *side_got),
        1,
    )


def solution(mesh):
    return jax.shard_map(
        local,
        mesh=mesh,
        in_specs=(P("row", "col", None), P(), P(), P()),
        out_specs=P("row", "col", None),
        check_vma=False,
    )
```

```python
import functools

import jax
import jax.numpy as jnp
from jax import lax
from jax.experimental import pallas as pl
from jax.experimental.pallas import tpu as pltpu
from jax.sharding import PartitionSpec as P


FAR = 64
DILATIONS = (1, 2, 4, 8)
PAD = 8
VMEM_LIMIT = 20 * 1024 * 1024


def normed(stream, gain):
    centre = jnp.mean(stream, axis=-1, keepdims=True)
    moved = stream - centre
    spread = jnp.mean(moved * moved, axis=-1, keepdims=True)
    return jax.nn.gelu(moved * lax.rsqrt(spread + 1e-05) * gain)


def spread_taps(line_ref, taps_ref, row, dilation, start, cols):
    ch = line_ref.shape[-1]
    for tap in range(3):
        shift = (tap - 1) * dilation
        taps_ref[row, :, tap * ch : (tap + 1) * ch] = line_ref[row, pl.ds(start + shift, cols), :].astype(
            taps_ref.dtype
        )


def clear_edges(line_ref):
    rows, width, ch = line_ref.shape
    line_ref[:, 0:PAD, :] = jnp.zeros((rows, PAD, ch), line_ref.dtype)
    line_ref[:, width - PAD : width, :] = jnp.zeros((rows, PAD, ch), line_ref.dtype)


def conv_part(taps_ref, weight_ref, first, rows, dilation, taps=(0, 1, 2)):
    cols, depth = taps_ref.shape[1:]
    lhs = [taps_ref[first + tap * dilation : first + tap * dilation + rows].reshape(rows * cols, depth) for tap in taps]
    lhs = lhs[0] if len(lhs) == 1 else jnp.concatenate(lhs, axis=1)
    weight = weight_ref[taps[0] * depth : (taps[-1] + 1) * depth, :]
    out = jnp.dot(lhs, weight, preferred_element_type=jnp.float32)
    return out.reshape(rows, cols, out.shape[-1])


def in_grid(col_lo, col_hi, value):
    cols = lax.broadcasted_iota(jnp.int32, value.shape, 0)
    keep = (cols >= col_lo) & (cols < col_hi)
    return jnp.where(keep, value, 0.0)


class Plan:
    def __init__(self, tile_rows, tile_cols, ch, n_row, n_col):
        self.tile_rows, self.tile_cols, self.ch = tile_rows, tile_cols, ch
        self.n_row, self.n_col = n_row, n_col
        self.two = n_col == 2
        self.ext = -(-sum(DILATIONS) // 16) * 16
        self.width = tile_cols + (self.ext if self.two else 2 * self.ext)
        self.last = DILATIONS[-1]
        self.width4 = tile_cols + (self.last if self.two else 2 * self.last)

    def own(self, col):
        return pl.multiple_of(col * self.ext, 8) if self.two else self.ext

    def own4(self, col):
        return pl.multiple_of(col * self.last, 8) if self.two else self.last

    def start4(self, col):
        return pl.multiple_of(col * (self.ext - self.last), 8) if self.two else self.ext - self.last

    def sides(self, col):
        if self.two:
            return (pl.multiple_of((1 - col) * self.tile_cols, 8),)
        return (0, self.ext + self.tile_cols)

    def edges(self, col):
        if self.two:
            return (pl.multiple_of((1 - col) * (self.tile_cols - self.ext), 16),)
        return self.tile_cols - self.ext, 0

    def col_range(self, col):
        if self.two:
            return 0, self.width
        lo = jnp.where(col == 0, self.ext, 0)
        hi = jnp.where(col == self.n_col - 1, self.ext + self.tile_cols, self.width)
        return lo, hi

    def inside(self, col, value):
        if self.two:
            return value
        return in_grid(*self.col_range(col), value)

    def starts(self, row_id, span):
        last = self.tile_rows - span
        one = jnp.where(row_id % 2 == 0, last, 0)
        return one, last - one


def lay(line, taps, row, value, dilation, start, cols):
    width = value.shape[0]
    line[row, PAD : PAD + width, :] = value
    spread_taps(line, taps, row, dilation, start, cols)


def rows_of(count, body, step=4):
    def block(k, _):
        for j in range(step):
            body(k * step + j)
        return 0

    lax.fori_loop(0, count // step, block, 0)
    for row in range(count // step * step, count):
        body(row)


def stage(plan, halo, features, *refs):
    n_side = 1 if plan.two else 2
    edges, outs, (sems,) = refs[:n_side], refs[n_side : 2 + n_side], refs[2 + n_side :]
    row_id, col = lax.axis_index("row"), lax.axis_index("col")
    moves = [(features.at[:, pl.ds(at, plan.ext)], edge) for at, edge in zip(plan.edges(col), edges)]
    moves += [(features.at[pl.ds(at, halo)], out) for at, out in zip(plan.starts(row_id, halo), outs)]
    copies = [pltpu.make_async_copy(src, dst, sems.at[k]) for k, (src, dst) in enumerate(moves)]
    for copy in copies:
        copy.start()
    for copy in copies:
        copy.wait()


def corners(plan, one, two, after, *refs):
    del after
    outs, (sems,) = refs[:-1], refs[-1:]
    col = lax.axis_index("col")
    halo = one.shape[0]
    copies = []
    for out, at in zip(outs, plan.edges(col)):
        for k, ref in enumerate((one, two)):
            copies.append(
                pltpu.make_async_copy(
                    ref.at[:, pl.ds(at, plan.ext)], out.at[pl.ds(k * halo, halo)], sems.at[len(copies)]
                )
            )
    for copy in copies:
        copy.start()
    for copy in copies:
        copy.wait()


CHUNK = 4


def one_prepare(plan, *refs):
    n_side = 1 if plan.two else 2
    features, sides = refs[0], refs[1 : 1 + n_side]
    gains_hbm, w_hbm, base, taps, w_one, gains, tile, line, sems = refs[1 + n_side :]
    moves = ((features, tile), (gains_hbm, gains), (w_hbm.at[0], w_one))
    copies = [pltpu.make_async_copy(src, dst, sems.at[k]) for k, (src, dst) in enumerate(moves)]
    for copy in copies:
        copy.start()
    col = lax.axis_index("col")
    parts = (tile,) + tuple(sides)
    clear_edges(line)
    for copy in copies[:2]:
        copy.wait()
    for part, offset in zip(parts, (plan.own(col),) + plan.sides(col)):
        base[:, pl.ds(offset, part.shape[1]), :] = part[...].astype(jnp.float32)

    def prepare(row):
        lay(line, taps, row, plan.inside(col, normed(base[row], gains[0:1, :])), DILATIONS[0], PAD, plan.width)

    rows_of(plan.tile_rows, prepare)
    copies[2].wait()


def fetch(w_hbm, layer, out, sem):
    return pltpu.make_async_copy(w_hbm.at[layer], out, sem)


def one_own(plan, base, taps, w_one, w_hbm, gains, mid, mid_act, w_next, sem):
    col = lax.axis_index("col")
    copy = fetch(w_hbm, 1, w_next, sem)
    copy.start()

    def follow(row):
        mid_act[row] = plan.inside(col, normed(mid[row], gains[1:2, :])).astype(mid_act.dtype)

    edge = DILATIONS[1]
    count = mid.shape[0] // CHUNK
    for k in range(count):
        at = k * CHUNK
        mid[at : at + CHUNK] = base[edge + at : edge + at + CHUNK] + conv_part(
            taps, w_one, edge + at - DILATIONS[0], CHUNK, DILATIONS[0]
        )
        if k:
            for row in range(at - CHUNK, at):
                follow(row)
    rows_of(CHUNK, lambda row: follow((count - 1) * CHUNK + row))
    copy.wait()


def one_two(plan, halo, *refs):
    n_side = 1 if plan.two else 2
    got, crossed, refs = refs[:2], refs[2 : 2 + n_side], refs[2 + n_side :]
    mid, mid_act, own_taps, own_base, w_one, w_two, w_hbm, gains = refs[:8]
    stream, taps_out, send_one, send_two, w_next = refs[8:13]
    base, line, taps_one, rim, taps_two, sem = refs[13:]
    line_out = line
    row_id, col = lax.axis_index("row"), lax.axis_index("col")
    copy = fetch(w_hbm, 2, w_next, sem)
    copy.start()
    rows, width, ch = plan.tile_rows, plan.width, plan.ch
    d_one, d_two = DILATIONS[:2]
    clear_edges(line)
    for k, first in enumerate((0, rows - halo)):
        at = (k + 1) * halo
        base[at : at + halo] = own_base[first : first + halo]
        taps_one[at : at + halo] = own_taps[first : first + halo]
    top = (halo * 3) * (1 - row_id % 2)
    for k, (ref, at) in enumerate(zip(got, (top, 3 * halo - top))):
        base[pl.ds(at, halo), pl.ds(plan.own(col), ref.shape[1]), :] = ref[...].astype(jnp.float32)
        for side, offset in zip(crossed, plan.sides(col)):
            base[pl.ds(at, halo), pl.ds(offset, side.shape[1]), :] = side[k * halo : (k + 1) * halo].astype(jnp.float32)
    for row in tuple(range(halo)) + tuple(range(3 * halo, 4 * halo)):
        lay(line, taps_one, row, plan.inside(col, normed(base[row], gains[0:1, :])), d_one, PAD, width)
    n_mid = mid.shape[0]

    def spread_mid(row):
        lay(line, taps_two, 2 * d_two + row, mid_act[row].astype(jnp.float32), d_two, PAD, width)

    for k in range(2):
        at = 2 * halo * k
        rim[k * CHUNK : (k + 1) * CHUNK] = base[at + 1 : at + 1 + CHUNK] + conv_part(taps_one, w_one, at, CHUNK, d_one)
        for row in range(k * n_mid // 2, (k + 1) * n_mid // 2):
            spread_mid(row)

    def spread_rim(row):
        value = plan.inside(col, normed(rim[row], gains[1:2, :]))
        if row < d_two:
            value = jnp.where(row_id == 0, 0.0, value)
        if row >= 2 * CHUNK - d_two:
            value = jnp.where(row_id == plan.n_row - 1, 0.0, value)
        lay(line, taps_two, row if row < CHUNK else n_mid + row, value, d_two, PAD, width)

    def finish(row):
        lay(line_out, taps_out, row, plan.inside(col, normed(stream[row], gains[2:3, :])), DILATIONS[2], PAD, width)

    def second(first):
        return conv_part(taps_two, w_two, first, CHUNK, d_two)

    inner = tuple(range(CHUNK, rows - CHUNK, CHUNK))
    per = -(-2 * CHUNK // len(inner))
    for k, first in enumerate(inner):
        stream[first : first + CHUNK] = mid[first - d_two : first - d_two + CHUNK] + second(first)
        for row in range(k * per, min((k + 1) * per, 2 * CHUNK)):
            spread_rim(row)
    out = second(0)
    stream[0:d_two] = rim[d_two : 2 * d_two] + out[:d_two]
    stream[d_two:CHUNK] = mid[0 : CHUNK - d_two] + out[d_two:]
    for first in inner[: len(inner) // 2]:
        for row in range(first, first + CHUNK):
            finish(row)
    last = rows - CHUNK
    out = second(last)
    stream[last : last + d_two] = mid[n_mid - d_two : n_mid] + out[:d_two]
    stream[last + d_two : rows] = rim[CHUNK : CHUNK + d_two] + out[d_two:]
    for first in inner[len(inner) // 2 :]:
        for row in range(first, first + CHUNK):
            finish(row)
    rows_of(CHUNK, finish)
    rows_of(CHUNK, lambda row: finish(last + row))
    for ref, at in zip((send_one, send_two), plan.starts(row_id, DILATIONS[2])):
        ref[...] = taps_out[pl.ds(at, DILATIONS[2]), :, ch : 2 * ch]
    copy.wait()


def three_own(plan, taps, weight, w_hbm, stream, gains, edge, mid, mid_act, w_next, full, row_act, sem):
    col = lax.axis_index("col")
    copy = fetch(w_hbm, 3, w_next, sem)
    copy.start()
    d = DILATIONS[2]
    rows = plan.tile_rows
    for first in range(d, rows - d, CHUNK):
        full[first - d : first - d + CHUNK] = stream[first : first + CHUNK] + conv_part(taps, weight, first - d, CHUNK, d)

    def finish(row):
        emit(plan, col, full, row_act, row, gains[3:4, :], mid, mid_act, row)

    count = rows - 2 * d
    edge[0:d] = stream[0:d] + conv_part(taps, weight, -d, d, d, (1, 2))
    for row in range(count // 2):
        finish(row)
    edge[d : 2 * d] = stream[rows - d : rows] + conv_part(taps, weight, rows - 2 * d, d, d, (0, 1))
    for row in range(count // 2, count):
        finish(row)
    copy.wait()


def emit(plan, col, full, row_act, row, gain, stream, act, at):
    row_act[row] = plan.inside(col, normed(full[row], gain))
    act[at] = row_act[row, pl.ds(plan.start4(col), plan.width4), :].astype(act.dtype)
    stream[at] = full[row, pl.ds(plan.own(col), plan.tile_cols), :]


def partner_weight(plan, row_id, k, weight):
    depth = 3 * plan.ch
    one = jnp.where(row_id % 2 == 0, 2 * depth, 0)
    return weight.at[pl.ds(pl.multiple_of((one, 2 * depth - one)[k], 128), depth)]


def three_rim(plan, got_one, got_two, edge, mid, mid_act, weight, gains, stream, act, send_one, send_two, *scratch):
    line, taps, full, row_act = scratch
    row_id, col = lax.axis_index("row"), lax.axis_index("col")
    d = DILATIONS[2]
    rows, width = plan.tile_rows, plan.width
    clear_edges(line)
    for k, ref in enumerate((got_one, got_two)):
        for row in range(d):
            lay(line, taps, k * d + row, ref[row].astype(jnp.float32), d, PAD, width)
    stream[d : rows - d] = mid[...]
    act[d : rows - d] = mid_act[...]
    at_one, at_two = plan.starts(row_id, d)
    half = jnp.where(row_id % 2 == 0, d, 0)
    for k, (place, at) in enumerate(((half, at_one), (d - half, at_two))):
        full[k * d : (k + 1) * d] = edge[pl.ds(place, d)] + conv_part(
            taps, partner_weight(plan, row_id, k, weight), k * d, d, d, (0,)
        )
    for k, at in enumerate((at_one, at_two)):
        for row in range(d):
            emit(plan, col, full, row_act, k * d + row, gains[3:4, :], stream, act, at + row)
    for ref, at in zip((send_one, send_two), plan.starts(row_id, DILATIONS[3])):
        ref[...] = act[pl.ds(at, DILATIONS[3])]


def four_own(plan, act, weight, stream, out, line, taps):
    col = lax.axis_index("col")
    d = DILATIONS[3]
    rows, cols = plan.tile_rows, plan.tile_cols
    start = PAD + plan.own4(col)
    clear_edges(line)
    rows_of(rows, lambda row: lay(line, taps, row, act[row].astype(jnp.float32), d, start, cols))
    for first in range(0, rows, CHUNK):
        used = tuple(t for t in range(3) if 0 <= first + (t - 1) * d < rows)
        out[first : first + CHUNK] = stream[first : first + CHUNK] + conv_part(taps, weight, first - d, CHUNK, d, used)


def four_rim(plan, k, got, acc, weight, gains, stream, act, line, taps):
    row_id, col = lax.axis_index("row"), lax.axis_index("col")
    d = DILATIONS[3]
    start = PAD + plan.own4(col)
    clear_edges(line)

    def spread(row):
        lay(line, taps, row, got[row].astype(jnp.float32), d, start, plan.tile_cols)

    def finish(row):
        act[row] = normed(stream[row], gains[4:5, :]).astype(act.dtype)

    for row in range(CHUNK):
        spread(row)
    at = plan.starts(row_id, d)[k]
    for first in range(0, d, CHUNK):
        stream[first : first + CHUNK] = acc[pl.ds(at + first, CHUNK)] + conv_part(
            taps, partner_weight(plan, row_id, k, weight), first, CHUNK, d, (0,)
        )
        if first:
            for row in range(first - CHUNK, first):
                finish(row)
        for row in range(first + CHUNK, min(first + 2 * CHUNK, d)):
            spread(row)
    for row in range(d - CHUNK, d):
        finish(row)


def times(a, w):
    rows, cols, ch = a.shape
    return jnp.dot(a.reshape(rows * cols, ch), w, preferred_element_type=jnp.float32).reshape(rows, cols, ch)


def call(kernel, out_shape, scratch, args, flops, any_args=(), out_space=pltpu.VMEM):
    return pl.pallas_call(
        kernel,
        out_shape=out_shape,
        in_specs=[
            pl.BlockSpec(memory_space=pltpu.HBM) if k in any_args else pl.BlockSpec(memory_space=pltpu.VMEM)
            for k in range(len(args))
        ],
        out_specs=jax.tree.map(lambda _: pl.BlockSpec(memory_space=out_space), out_shape),
        scratch_shapes=scratch,
        compiler_params=pltpu.CompilerParams(vmem_limit_bytes=VMEM_LIMIT),
        cost_estimate=pl.CostEstimate(flops=int(flops), transcendentals=0, bytes_accessed=0),
    )(*args)


def taps_sent(plan, col):
    return (2 * col,) if plan.two else (0, 2)


def taps_got(plan, col):
    return (2 - 2 * col,) if plan.two else (0, 2)


def far_rows(plan):
    group = lax.axis_index("row") // (FAR // plan.tile_rows)
    one = 2 - 2 * (group % 2)
    return one, 2 - one


def far_a(plan, a, w, stream, part_one, part_two, own):
    one, two = far_rows(plan)
    part_one[...] = times(a[...], w[two, 1])
    part_two[...] = times(a[...], w[one, 1])
    own[...] = stream[...] + times(a[...], w[1, 1])


def far_b(plan, b, w, stream, own, *side):
    col = lax.axis_index("col")
    own[...] = stream[...] + times(b[...], w[1, 1])
    for ref, tap in zip(side, taps_sent(plan, col)):
        ref[...] = times(b[...], w[1, tap])


def far_two(plan, n_side, *refs):
    crossed = refs[:n_side]
    got_one, got_two, w, part_one, part_two = refs[n_side : n_side + 5]
    side_b = refs[n_side + 5 : 2 * n_side + 5]
    out_one, out_two = refs[2 * n_side + 5 : 2 * n_side + 7]
    side_out = refs[2 * n_side + 7 :]
    col = lax.axis_index("col")
    one, two = far_rows(plan)
    for part, out, tap_row in ((part_one, out_one, two), (part_two, out_two, one)):
        total = part[...]
        for ref, tap in zip(crossed, taps_got(plan, col)):
            total = total + times(ref[...], w[tap_row, tap])
        out[...] = total.astype(out.dtype)
    for ref, acc, tap in zip(side_out, side_b, taps_sent(plan, col)):
        ref[...] = (acc[...] + times(got_one[...], w[one, tap]) + times(got_two[...], w[two, tap])).astype(ref.dtype)


def far_three(plan, n_side, *refs):
    crossed = refs[:n_side]
    got_one, got_two, w, own_a, own_b, out_a, out_b = refs[n_side:]
    col = lax.axis_index("col")
    one, two = far_rows(plan)
    total = own_a[...]
    for ref, tap in zip(crossed, taps_got(plan, col)):
        total = total + times(ref[...], w[1, tap])
    out_a[...] = total
    out_b[...] = own_b[...] + times(got_one[...], w[one, 1]) + times(got_two[...], w[two, 1])


def far_four(plan, n_side, own_a, own_b, back_one, back_two, *refs):
    side_b, (out_ref, held, sems) = refs[:n_side], refs[n_side:]
    half = own_a.shape[0]
    at_a, at_b = plan.starts(lax.axis_index("row"), half)
    copies = [
        pltpu.make_async_copy(held.at[k], out_ref.at[pl.ds(at, half)], sems.at[k]) for k, at in enumerate((at_a, at_b))
    ]
    held[0] = own_a[...] + back_one[...].astype(jnp.float32) + back_two[...].astype(jnp.float32)
    copies[0].start()
    total = own_b[...]
    for ref in side_b:
        total = total + ref[...].astype(jnp.float32)
    held[1] = total
    copies[1].start()
    for copy in copies:
        copy.wait()


def pair(value, hop, parity):
    n_row, n_col = lax.axis_size("row"), lax.axis_size("col")
    ups = [
        (r * n_col + c, (r + hop) * n_col + c)
        for r in range(n_row - hop)
        for c in range(n_col)
        if r // hop % 2 == parity
    ]
    return lax.ppermute(value, ("row", "col"), ups + [(j, i) for i, j in ups])


def row_swap(one, two):
    got_two = pair(two, 1, 1)
    got_one = pair(one, 1, 0)
    return got_one, got_two


def move(value, rows, cols):
    n_row, n_col = lax.axis_size("row"), lax.axis_size("col")
    pairs = [
        (r * n_col + c, (r + rows) * n_col + c + cols)
        for r in range(n_row)
        for c in range(n_col)
        if 0 <= r + rows < n_row and 0 <= c + cols < n_col
    ]
    return lax.ppermute(value, ("row", "col"), pairs)


def cross(value):
    return lax.ppermute(value, "col", [(0, 1), (1, 0)])


def local(features, inner_weights, far_weights, gains):
    tile_rows, tile_cols, ch = features.shape
    plan = Plan(tile_rows, tile_cols, ch, lax.axis_size("row"), lax.axis_size("col"))
    d_one, d_two, d_three, d_four = DILATIONS
    halo = d_one + d_two
    ext, width, width4 = plan.ext, plan.width, plan.width4
    bf16, f32 = jnp.bfloat16, jnp.float32
    shape, vmem, dma = jax.ShapeDtypeStruct, pltpu.VMEM, pltpu.SemaphoreType.DMA
    features, gains = [pltpu.with_memory_space_constraint(value, pltpu.HBM) for value in (features, gains)]
    weights = pltpu.with_memory_space_constraint(inner_weights.reshape(inner_weights.shape[0], 9 * ch, ch), pltpu.HBM)
    n_side = 1 if plan.two else 2
    halo_shape, edge_shape = shape((halo, tile_cols, ch), bf16), shape((tile_rows, ext, ch), bf16)
    refs = call(
        functools.partial(stage, plan, halo),
        [edge_shape] * n_side + [halo_shape] * 2,
        [dma((2 + n_side,))],
        (features,),
        1,
        any_args=(0,),
    )
    edges, (one, two) = refs[:n_side], refs[n_side:]

    def spread_sides(values):
        if plan.two:
            return [cross(values[0])]
        return [move(values[0], 0, 1), move(values[1], 0, -1)]

    sides = spread_sides(edges)
    got_one, got_two = row_swap(one, two)
    per_row = 2 * 9 * ch * ch
    whole = 9 * ch
    n_mid = tile_rows - 2 * d_two
    line = vmem((tile_rows, width + 2 * PAD, ch), f32)
    taps = vmem((tile_rows, width, 3 * ch), bf16)
    w_shape = shape((whole, ch), bf16)
    base, taps1, w_one, gains = call(
        functools.partial(one_prepare, plan),
        (shape((tile_rows, width, ch), f32), shape((tile_rows, width, 3 * ch), bf16), w_shape, shape(gains.shape, f32)),
        [vmem(features.shape, bf16), line, dma((3,))],
        (features, *sides, gains, weights),
        per_row * 8 * width,
        any_args=(0, 1 + n_side, 2 + n_side),
    )
    crossed = spread_sides(
        call(
            functools.partial(corners, plan),
            [shape((2 * halo, ext, ch), bf16)] * n_side,
            [dma((2 * n_side,))],
            (got_one, got_two, taps1),
            1,
            any_args=(2,),
        )
    )
    mid, mid_act, w_two = call(
        functools.partial(one_own, plan),
        (shape((n_mid, width, ch), f32), shape((n_mid, width, ch), bf16), w_shape),
        [dma],
        (base, taps1, w_one, weights, gains),
        per_row * n_mid * width,
        any_args=(3,),
    )
    sent = shape((d_three, width, ch), bf16)
    stream2, taps3, one, two, w_three = call(
        functools.partial(one_two, plan, halo),
        (shape((tile_rows, width, ch), f32), shape((tile_rows, width, 3 * ch), bf16), sent, sent, w_shape),
        [
            vmem((4 * halo, width, ch), f32),
            vmem((n_mid + 2 * CHUNK, width + 2 * PAD, ch), f32),
            vmem((4 * halo, width, 3 * ch), bf16),
            vmem((2 * CHUNK, width, ch), f32),
            vmem((n_mid + 2 * CHUNK, width, 3 * ch), bf16),
            dma,
        ],
        (got_one, got_two, *crossed, mid, mid_act, taps1, base, w_one, w_two, weights, gains),
        per_row * (2 * CHUNK + tile_rows) * width,
        any_args=(8 + n_side,),
    )
    got_one, got_two = row_swap(one, two)
    n_mid = tile_rows - 2 * d_three
    row_f32 = vmem((tile_rows, width, ch), f32)
    edge, mid, mid_act, w_four = call(
        functools.partial(three_own, plan),
        (
            shape((2 * d_three, width, ch), f32),
            shape((n_mid, tile_cols, ch), f32),
            shape((n_mid, width4, ch), bf16),
            w_shape,
        ),
        [row_f32, row_f32, dma],
        (taps3, w_three, weights, stream2, gains),
        per_row * tile_rows * width,
        any_args=(2,),
    )
    sent = shape((d_four, width4, ch), bf16)
    stream3, act4, one, two = call(
        functools.partial(three_rim, plan),
        (shape((tile_rows, tile_cols, ch), f32), shape((tile_rows, width4, ch), bf16), sent, sent),
        [
            vmem((2 * d_three, width + 2 * PAD, ch), f32),
            vmem((2 * d_three, width, 3 * ch), bf16),
            vmem((2 * d_three, width, ch), f32),
            vmem((2 * d_three, width, ch), f32),
        ],
        (got_one, got_two, edge, mid, mid_act, w_three, gains),
        per_row * 2 * d_three * width / 3,
    )
    got_one, got_two = row_swap(one, two)
    line = vmem((tile_rows, width4 + 2 * PAD, ch), f32)
    taps = vmem((tile_rows, tile_cols, 3 * ch), bf16)
    acc4 = call(
        functools.partial(four_own, plan),
        shape((tile_rows, tile_cols, ch), f32),
        [line, taps],
        (act4, w_four, stream3),
        per_row * tile_rows * tile_cols,
    )
    half = tile_rows // 2
    if half != d_four or FAR // tile_rows % 2:
        raise ValueError("tile rows")
    finished = [
        call(
            functools.partial(four_rim, plan, k),
            (shape((half, tile_cols, ch), f32), shape((half, tile_cols, ch), bf16)),
            [
                vmem((d_four, width4 + 2 * PAD, ch), f32),
                vmem((d_four, tile_cols, 3 * ch), bf16),
            ],
            (got, acc4, w_four, gains),
            per_row * d_four * tile_cols / 3,
        )
        for k, got in enumerate((got_one, got_two))
    ]
    (stream_a, a), (stream_b, b) = finished
    row_hop, col_hop = FAR // tile_rows, FAR // tile_cols
    if plan.two:
        crossed = [cross(a)]
    else:
        crossed = [move(a, 0, col_hop), move(a, 0, -col_hop)]
    got_one, got_two = pair(b, row_hop, 0), pair(b, row_hop, 1)
    block = shape((half, tile_cols, ch), f32)
    sent = shape((half, tile_cols, ch), bf16)
    per_half = 2 * ch * ch * half * tile_cols
    part_one, part_two, own_a = call(
        functools.partial(far_a, plan), [block] * 3, [], (a, far_weights, stream_a), per_half * 3
    )
    own_b, *side_b = call(
        functools.partial(far_b, plan), [block] * (1 + n_side), [], (b, far_weights, stream_b), per_half * 2
    )
    one, two, *sides = call(
        functools.partial(far_two, plan, n_side),
        [sent] * (2 + n_side),
        [],
        (*crossed, got_one, got_two, far_weights, part_one, part_two, *side_b),
        per_half * 4,
    )
    back_one, back_two = pair(one, row_hop, 0), pair(two, row_hop, 1)
    if plan.two:
        side_got = [cross(sides[0])]
    else:
        side_got = [move(sides[0], 0, col_hop), move(sides[1], 0, -col_hop)]
    own_a, own_b = call(
        functools.partial(far_three, plan, n_side),
        [block] * 2,
        [],
        (*crossed, got_one, got_two, far_weights, own_a, own_b),
        per_half * 3,
    )
    return call(
        functools.partial(far_four, plan, n_side),
        shape((tile_rows, tile_cols, ch), f32),
        [vmem((2, half, tile_cols, ch), f32), dma((2,))],
        (own_a, own_b, back_one, back_two, *side_got),
        1,
        out_space=pltpu.HBM,
    )


def solution(mesh):
    return jax.shard_map(
        local,
        mesh=mesh,
        in_specs=(P("row", "col", None), P(), P(), P()),
        out_specs=P("row", "col", None),
        check_vma=False,
    )
```
